32 devices in a mesh: groups: 2 (over y), col: 16 (over z, x, core).
Axes of the slice: x: 2, y: 2, z: 4, core: 2. Of those that a mesh axis runs over, the one named last changes fastest.
Arguments:
- fields: bfloat16 [32, 137, 2048], P(('groups', 'col')), parts along dimension 0, may hold values from -6 to 6
- level_count: int32 [2048], replicated, may hold values from 68 to 137
- owner: int32 [16], replicated, may hold values from 0 to 15, as said below
- band_start: int32 [16, 37], replicated, may hold values from 0 to 133
- interp_weights: float32 [16, 37, 4], replicated, may hold values from -3 to 3
Outputs:
- timemajor: bfloat16 [32, 37, 2048], P(('groups', 'col')), parts along dimension 0
- series: bfloat16 [96, 37, 16, 128], P(('groups', 'col')), parts along dimension 0
The draws below stay inside these ranges and needn't reach their ends.
There are 2 independent parts, one for each index of `groups`. The reference program is written for one: setup_inputs(seed, part) draws one part's arguments, and reference() takes and returns one part's arrays. A program takes and returns all parts, laid end to end along the dimension named above; an argument that names none is the same for every part. Nothing has to cross between parts.
Inputs may be any that keep to these rules, and one draw needn't show every extreme that they name: No owner holds more than 3 blocks, and some owner holds exactly 3.
All inputs are finite; a program needn't handle non-finite values.
Results may differ from the reference program's by a relative error of at most 0.0085.
Values may be sent and summed in bfloat16 or wider, within the bound.
A program may use at most 64 MiB of HBM per device.

```python
import jax
import jax.numpy as jnp
from jax import lax

LEV = 137
PLEV = 37
BAND = 4
CBLK = 128
MOST = 3
TIMES = 16
BLOCKS = 16
COLS = 2048
N_COL = 16


def draw_owner(key, part):
    total = N_COL * MOST
    first, second, third = jax.random.split(jax.random.fold_in(key, 11), 3)
    chosen = jax.random.randint(first, (), 0, N_COL)
    order = jax.random.permutation(second, total).astype(jnp.int32)
    slot_index = jnp.arange(total, dtype=jnp.int32)
    slot_owner = slot_index // MOST
    at_ends = (slot_index == 0) | (slot_index == (N_COL - 1) * MOST)
    score = jnp.where(slot_owner == chosen, order - 3 * total, jnp.where(at_ends, order - 2 * total, order))
    picked = jnp.argsort(score, stable=True)[:N_COL]
    owners = (picked // MOST).astype(jnp.int32)
    shuffle = jax.random.permutation(third, N_COL)
    return owners[shuffle].astype(jnp.int32)


def set_ends(values, rng, low, high):
    longest = values.shape.index(max(values.shape))
    spots = []
    for shift in (0, 1):
        where = [jax.random.randint(jax.random.fold_in(rng, axis), (), 0, length) for axis, length in enumerate(values.shape)]
        where[longest] = (where[longest] + shift) % values.shape[longest]
        spots.append(tuple(where))
    return values.at[spots[0]].set(low).at[spots[1]].set(high)


def block_levels(stream_key, shape, cuts, low, top_value):
    def one(axis_at, parts):
        heights = jax.random.uniform(jax.random.fold_in(jax.random.fold_in(stream_key, 6), axis_at), (parts,), jnp.float32, low / len(cuts), top_value / len(cuts))
        return jnp.repeat(jnp.exp(heights), shape[axis_at] // parts).reshape((-1,) + (1,) * (len(shape) - axis_at - 1))

    factor_of = one(*cuts[0])
    for cut in cuts[1:]:
        factor_of = factor_of * one(*cut)
    return factor_of


def centred(key, shape, scale, limit, cuts=(), held_as=jnp.bfloat16):
    values = jax.random.normal(key, shape, jnp.float32) * scale
    if len(cuts) > 0:
        values = block_levels(key, shape, cuts, -0.22, 0.18) * values
    return jnp.clip(values, min=-limit, max=limit).astype(held_as)


def setup_inputs(seed: int = 0, part: int = 0) -> dict:
    arg_keys = jax.random.split(jax.random.key(seed), 6)
    part_keys = jax.random.split(jax.random.fold_in(arg_keys[5], part), 6)
    return {
        "fields": centred(part_keys[0], (TIMES, LEV, COLS), 1.0, 6.0, ((0, 16),)),
        "level_count": set_ends(jax.random.randint(arg_keys[1], (COLS,), LEV // 2, LEV + 1), jax.random.fold_in(arg_keys[1], 1), LEV // 2, LEV).astype(jnp.int32),
        "owner": draw_owner(jax.random.fold_in(arg_keys[5], 71), part),
        "band_start": set_ends(jax.random.randint(arg_keys[3], (BLOCKS, PLEV), 0, LEV - BAND + 1), jax.random.fold_in(arg_keys[3], 1), 0, LEV - BAND).astype(jnp.int32),
        "interp_weights": centred(arg_keys[4], (BLOCKS, PLEV, BAND), BAND ** -0.5, 3.0, (), jnp.float32),
    }


def fill_levels(block, counts):
    lev = jnp.arange(LEV, dtype=jnp.int32)[:, None]
    last = jnp.sum(jnp.where(lev == counts[None, :] - 1, block.astype(jnp.float32), 0.0), axis=1, keepdims=True)
    return jnp.where(lev < counts[None, :], block, last.astype(jnp.bfloat16))


def level_matrix(weights, starts):
    lev = jnp.arange(LEV, dtype=jnp.int32)
    offsets = jnp.arange(BAND, dtype=jnp.int32)
    hit = lev[None, None, :] == (starts[:, None] + offsets[None, :])[:, :, None]
    return jnp.sum(weights[:, :, None] * hit.astype(jnp.float32), axis=1).astype(jnp.bfloat16)


def reference(fields, level_count, owner, band_start, interp_weights):
    times = fields.shape[0]
    blocks = owner.shape[0]
    grouped = jnp.moveaxis(fields.reshape(times, LEV, blocks, CBLK), 2, 0)
    counts = level_count.reshape(blocks, CBLK)

    def one_block(items):
        block, count_row, weights, starts = items
        filled = fill_levels(block, count_row)
        matrix = level_matrix(weights, starts)
        result = jnp.einsum("pl,tlc->tpc", matrix.astype(jnp.float32), filled.astype(jnp.float32))
        return result.astype(jnp.bfloat16)

    results = lax.map(one_block, (grouped, counts, interp_weights, band_start))
    timemajor = jnp.moveaxis(results, 0, 2).reshape(times, PLEV, blocks * CBLK)
    onehot = (owner[:, None] == jnp.arange(N_COL, dtype=jnp.int32)[None, :]).astype(jnp.int32)
    before = jnp.cumsum(onehot, axis=0) - onehot
    slot = jnp.sum(before * onehot, axis=1).astype(jnp.int32)
    global_slot = (owner * MOST + slot).astype(jnp.int32)
    series = jnp.zeros((N_COL * MOST, PLEV, times, CBLK), jnp.bfloat16)
    series = series.at[global_slot].set(jnp.transpose(results, (0, 2, 1, 3)))
    return timemajor, series
```

```python
import functools

import jax
import jax.numpy as jnp
from jax import lax
from jax.experimental import pallas as pl
from jax.experimental.pallas import tpu as pltpu
from jax.sharding import PartitionSpec as P

LEV = 137
PLEV = 37
BAND = 4
CBLK = 128
MOST = 3
LOW = (LEV // 2 - 1) // 16 * 16
ROWS = -(-MOST * PLEV // 8) * 8
CHUNKS = 4


def loop(count, body):
    if count <= 16:
        for i in range(count):
            body(i)
    else:

        def step(i, carry):
            body(i)
            return carry

        lax.fori_loop(0, count, step, 0)


def partner(me, k, n):
    if n & (n - 1):
        return (me + k) % n
    other = me
    bit = 1
    while bit < n:
        flip = (k // bit) % 2
        other = other + flip * bit * (1 - 2 * ((me // bit) % 2))
        bit *= 2
    return other


def kernel(n, blocks, fields, counts, owner, starts, weights, tm, arrived,
           data, res, stage, packed, table, load_sem, send_sem, recv_sem):
    me = lax.axis_index("col")
    width = data.shape[1] // CHUNKS
    loads = []
    for i in range(CHUNKS):
        span = pl.ds(i * width, width)
        load = pltpu.make_async_copy(fields.at[0, :, span], data.at[:, span], load_sem.at[i])
        load.start()
        loads.append(load)

    barrier = pltpu.get_barrier_semaphore()

    def greet(i):
        pl.semaphore_signal(
            barrier, inc=1, device_id={"col": partner(me, n - 1 - i, n)},
            device_id_type=pl.DeviceIdType.MESH,
        )

    loop(n - 1, greet)

    def find(d):
        seen = jnp.int32(0)
        found = [jnp.int32(blocks)] * MOST

        def look(b, carry):
            seen, found = carry
            hit = owner[b] == d
            found = [jnp.where(hit & (seen == s), b, f) for s, f in enumerate(found)]
            return seen + hit.astype(jnp.int32), found

        if blocks <= 16:
            for b in range(blocks):
                seen, found = look(b, (seen, found))
        else:
            seen, found = lax.fori_loop(0, blocks, look, (seen, found))
        for s in range(MOST):
            table[d * MOST + s] = found[s]

    loop(n, find)

    res[blocks] = jnp.zeros(res.shape[1:], jnp.float32)
    stage[...] = jnp.zeros_like(stage)

    def interpolate(b):
        cols = pl.ds(pl.multiple_of(b * CBLK, CBLK), CBLK)
        count = counts[pl.ds(b, 1), :]
        high = data[LOW:, cols].astype(jnp.float32)
        lev = LOW + lax.broadcasted_iota(jnp.int32, high.shape, 0)
        last = jnp.sum(jnp.where(lev == count - 1, high, 0.0), axis=0, keepdims=True)
        high = jnp.where(lev < count, high, last).astype(jnp.bfloat16)
        filled = jnp.concatenate([data[:LOW, cols], high], axis=0)
        start = starts[pl.ds(b, 1), :]
        offset = lax.broadcasted_iota(jnp.int32, (LEV, PLEV), 0) - start
        matrix = jnp.zeros((LEV, PLEV), jnp.float32)
        for k in range(BAND):
            matrix = jnp.where(offset == k, weights[b, pl.ds(k, 1), :], matrix)
        out = lax.dot_general(
            matrix.astype(jnp.bfloat16), filled, (((0,), (0,)), ((), ())),
            preferred_element_type=jnp.float32,
        )
        res[b, :PLEV] = out
        tm[0, :, cols] = out.astype(jnp.bfloat16)

    per = blocks // CHUNKS
    for i in range(CHUNKS):
        loads[i].wait()
        if blocks <= 16:
            for b in range(i * per, (i + 1) * per):
                interpolate(b)
        else:
            def step(b, carry, i=i):
                interpolate(b + i * per)
                return carry

            lax.fori_loop(0, per, step, 0)

    def pack(d):
        for s in range(MOST):
            stage[s * PLEV:(s + 1) * PLEV] = res[table[d * MOST + s], :PLEV]
        return stage[...].astype(jnp.bfloat16)

    pl.semaphore_wait(barrier, n - 1)

    def copy_to(k):
        d = partner(me, k, n)
        return pltpu.make_async_remote_copy(
            src_ref=packed.at[k], dst_ref=arrived.at[me],
            send_sem=send_sem.at[k], recv_sem=recv_sem.at[me],
            device_id={"col": d}, device_id_type=pl.DeviceIdType.MESH,
        )

    def send(i):
        k = n - 1 - i
        packed[k] = pack(partner(me, k, n))
        copy_to(k).start()

    loop(n - 1, send)
    arrived[me] = pack(me)

    def finish(i):
        k = i + 1
        src = partner(me, k, n) if not (n & (n - 1)) else (me + n - k) % n
        pltpu.make_async_remote_copy(
            src_ref=packed.at[k], dst_ref=arrived.at[src],
            send_sem=send_sem.at[k], recv_sem=recv_sem.at[src],
            device_id={"col": src}, device_id_type=pl.DeviceIdType.MESH,
        ).wait_recv()
        copy_to(k).wait_send()

    loop(n - 1, finish)


def per_device(fields, level_count, owner, band_start, interp_weights):
    n = lax.axis_size("col")
    blocks = owner.shape[0]
    vmem = pl.BlockSpec(memory_space=pltpu.VMEM)
    timemajor, arrived = pl.pallas_call(
        functools.partial(kernel, n, blocks),
        out_shape=(
            jax.ShapeDtypeStruct((1, PLEV, blocks * CBLK), jnp.bfloat16),
            jax.ShapeDtypeStruct((n, ROWS, CBLK), jnp.bfloat16),
        ),
        in_specs=[
            pl.BlockSpec(memory_space=pl.ANY), vmem,
            pl.BlockSpec(memory_space=pltpu.SMEM), vmem, vmem,
        ],
        out_specs=(vmem, vmem),
        scratch_shapes=[
            pltpu.VMEM((LEV, blocks * CBLK), jnp.bfloat16),
            pltpu.VMEM((blocks + 1, -(-PLEV // 8) * 8, CBLK), jnp.float32),
            pltpu.VMEM((ROWS, CBLK), jnp.float32),
            pltpu.VMEM((n, ROWS, CBLK), jnp.bfloat16),
            pltpu.SMEM((n * MOST,), jnp.int32),
            pltpu.SemaphoreType.DMA((CHUNKS,)),
            pltpu.SemaphoreType.DMA((n,)),
            pltpu.SemaphoreType.DMA((n,)),
        ],
        compiler_params=pltpu.CompilerParams(collective_id=0, has_side_effects=True),
    )(
        fields, level_count.reshape(blocks, CBLK), owner, band_start,
        jnp.swapaxes(interp_weights, 1, 2),
    )
    series = arrived[:, :MOST * PLEV].reshape(n, MOST, PLEV, CBLK)
    return (timemajor, jnp.transpose(series, (1, 2, 0, 3)))


def solution(mesh):
    placed = (P(("groups", "col"), None, None), P(), P(), P(), P())
    return jax.shard_map(
        per_device,
        mesh=mesh,
        in_specs=placed,
        out_specs=(P(("groups", "col"), None, None), P(("groups", "col"), None, None, None)),
        check_vma=False,
    )
```

```python
import functools

import jax
import jax.numpy as jnp
from jax import lax
from jax.experimental import pallas as pl
from jax.experimental.pallas import tpu as pltpu
from jax.sharding import PartitionSpec as P

LEV = 137
PLEV = 37
BAND = 4
CBLK = 128
MOST = 3
LOW = (LEV // 2 - 1) // 16 * 16
ROWS = -(-MOST * PLEV // 8) * 8
CHUNKS = 4


def loop(count, body):
    if count <= 16:
        for i in range(count):
            body(i)
    else:

        def step(i, carry):
            body(i)
            return carry

        lax.fori_loop(0, count, step, 0)


def partner(me, k, n):
    return (me + k) % n
    other = me
    bit = 1
    while bit < n:
        flip = (k // bit) % 2
        other = other + flip * bit * (1 - 2 * ((me // bit) % 2))
        bit *= 2
    return other


def kernel(n, blocks, fields, counts_in, owner_in, starts_in, weights_in, tm_out, arrived,
           data, counts, owner, starts, weights, tm, res, stage, packed, table,
           load_sem, small_sem, out_sem, send_sem, recv_sem):
    me = lax.axis_index("col")
    barrier = pltpu.get_barrier_semaphore()

    def greet(i):
        pl.semaphore_signal(
            barrier, inc=1, device_id={"col": partner(me, n - 1 - i, n)},
            device_id_type=pl.DeviceIdType.MESH,
        )

    loop(n - 1, greet)

    smalls = []
    for i, (src, dst) in enumerate(
        [(owner_in, owner), (counts_in, counts), (starts_in, starts), (weights_in, weights)]
    ):
        small = pltpu.make_async_copy(src, dst, small_sem.at[i])
        small.start()
        smalls.append(small)
    width = data.shape[1] // CHUNKS
    loads = []
    for i in range(CHUNKS):
        span = pl.ds(i * width, width)
        load = pltpu.make_async_copy(fields.at[0, :, span], data.at[:, span], load_sem.at[i])
        load.start()
        loads.append(load)

    smalls[0].wait()

    def find(d):
        seen = jnp.int32(0)
        found = [jnp.int32(blocks)] * MOST

        def look(b, carry):
            seen, found = carry
            hit = owner[b] == d
            found = [jnp.where(hit & (seen == s), b, f) for s, f in enumerate(found)]
            return seen + hit.astype(jnp.int32), found

        if blocks <= 16:
            for b in range(blocks):
                seen, found = look(b, (seen, found))
        else:
            seen, found = lax.fori_loop(0, blocks, look, (seen, found))
        for s in range(MOST):
            table[d * MOST + s] = found[s]

    loop(n, find)

    res[blocks] = jnp.zeros(res.shape[1:], jnp.float32)
    stage[...] = jnp.zeros_like(stage)

    def interpolate(b):
        cols = pl.ds(pl.multiple_of(b * CBLK, CBLK), CBLK)
        count = counts[pl.ds(b, 1), :]
        high = data[LOW:, cols].astype(jnp.float32)
        lev = LOW + lax.broadcasted_iota(jnp.int32, high.shape, 0)
        last = jnp.sum(jnp.where(lev == count - 1, high, 0.0), axis=0, keepdims=True)
        high = jnp.where(lev < count, high, last).astype(jnp.bfloat16)
        filled = jnp.concatenate([data[:LOW, cols], high], axis=0)
        start = starts[pl.ds(b, 1), :]
        offset = lax.broadcasted_iota(jnp.int32, (LEV, PLEV), 0) - start
        matrix = jnp.zeros((LEV, PLEV), jnp.float32)
        for k in range(BAND):
            matrix = jnp.where(offset == k, weights[b, pl.ds(k, 1), :], matrix)
        out = lax.dot_general(
            matrix.astype(jnp.bfloat16), filled, (((0,), (0,)), ((), ())),
            preferred_element_type=jnp.float32,
        )
        res[b, :PLEV] = out
        tm[0, :, cols] = out.astype(jnp.bfloat16)

    for small in smalls[1:]:
        small.wait()
    per = blocks // CHUNKS
    for i in range(CHUNKS):
        loads[i].wait()
        if blocks <= 16:
            for b in range(i * per, (i + 1) * per):
                interpolate(b)
        else:
            def step(b, carry, i=i):
                interpolate(b + i * per)
                return carry

            lax.fori_loop(0, per, step, 0)

    def pack(d):
        for s in range(MOST):
            stage[s * PLEV:(s + 1) * PLEV] = res[table[d * MOST + s], :PLEV]
        return stage[...].astype(jnp.bfloat16)

    tm_copy = pltpu.make_async_copy(tm, tm_out, out_sem.at[0])
    tm_copy.start()

    def copy_to(k):
        d = partner(me, k, n)
        return pltpu.make_async_remote_copy(
            src_ref=packed.at[k], dst_ref=arrived.at[me],
            send_sem=send_sem.at[k], recv_sem=recv_sem.at[me],
            device_id={"col": d}, device_id_type=pl.DeviceIdType.MESH,
        )

    def fill(k):
        packed[k] = pack(partner(me, k, n))

    loop(n, fill)
    own = pltpu.make_async_copy(packed.at[0], arrived.at[me], out_sem.at[1])
    own.start()
    pl.semaphore_wait(barrier, n - 1)

    def order(i):
        return i + 1

    def send(i):
        copy_to(order(i)).start()

    loop(n - 1, send)

    def finish(i):
        k = i + 1
        src = (me + n - k) % n
        pltpu.make_async_remote_copy(
            src_ref=packed.at[k], dst_ref=arrived.at[src],
            send_sem=send_sem.at[k], recv_sem=recv_sem.at[src],
            device_id={"col": src}, device_id_type=pl.DeviceIdType.MESH,
        ).wait_recv()
        copy_to(k).wait_send()

    loop(n - 1, finish)
    own.wait()
    tm_copy.wait()


def per_device(fields, level_count, owner, band_start, interp_weights):
    n = lax.axis_size("col")
    blocks = owner.shape[0]
    anywhere = pl.BlockSpec(memory_space=pl.ANY)
    cols = blocks * CBLK
    tall = -(-PLEV // 8) * 8
    grant = 2 * cols * (LEV + PLEV + 18) + 4 * CBLK * tall * (blocks + 1) + 2 * n * ROWS * CBLK
    grant += blocks * 12 * CBLK * 4 + (3 << 20)
    timemajor, arrived = pl.pallas_call(
        functools.partial(kernel, n, blocks),
        out_shape=(
            jax.ShapeDtypeStruct((1, PLEV, cols), jnp.bfloat16),
            jax.ShapeDtypeStruct((n, ROWS, CBLK), jnp.bfloat16),
        ),
        in_specs=[pl.BlockSpec(memory_space=pltpu.HBM)] * 5,
        out_specs=(anywhere, anywhere),
        scratch_shapes=[
            pltpu.VMEM((LEV, cols), jnp.bfloat16),
            pltpu.VMEM((blocks, CBLK), jnp.int32),
            pltpu.SMEM((blocks,), jnp.int32),
            pltpu.VMEM((blocks, PLEV), jnp.int32),
            pltpu.VMEM((blocks, BAND, PLEV), jnp.float32),
            pltpu.VMEM((1, PLEV, cols), jnp.bfloat16),
            pltpu.VMEM((blocks + 1, tall, CBLK), jnp.float32),
            pltpu.VMEM((ROWS, CBLK), jnp.float32),
            pltpu.VMEM((n, ROWS, CBLK), jnp.bfloat16),
            pltpu.SMEM((n * MOST,), jnp.int32),
            pltpu.SemaphoreType.DMA((CHUNKS,)),
            pltpu.SemaphoreType.DMA((4,)),
            pltpu.SemaphoreType.DMA((2,)),
            pltpu.SemaphoreType.DMA((n,)),
            pltpu.SemaphoreType.DMA((n,)),
        ],
        compiler_params=pltpu.CompilerParams(
            collective_id=0, has_side_effects=True, vmem_limit_bytes=grant
        ),
    )(
        *[pltpu.with_memory_space_constraint(x, pltpu.HBM) for x in (
            fields, level_count.reshape(blocks, CBLK), owner, band_start,
            jnp.swapaxes(interp_weights, 1, 2),
        )]
    )
    series = arrived[:, :MOST * PLEV].reshape(n, MOST, PLEV, CBLK)
    return (timemajor, jnp.transpose(series, (1, 2, 0, 3)))


def solution(mesh):
    placed = (P(("groups", "col"), None, None), P(), P(), P(), P())
    return jax.shard_map(
        per_device,
        mesh=mesh,
        in_specs=placed,
        out_specs=(P(("groups", "col"), None, None), P(("groups", "col"), None, None, None)),
        check_vma=False,
    )
```
